32 devices in a mesh: ctx: 4 (over z), ep: 8 (over y, x, core).
Axes of the slice: x: 2, y: 2, z: 4, core: 2. Of those that a mesh axis runs over, the one named last changes fastest.
Arguments:
- out_grad: bfloat16 [64, 3584], P(('ctx', 'ep')), may hold values from -6 to 6
- expert_ids: int32 [64, 8], P(('ctx', 'ep')), may hold values from 0 to 31, all different within a row; in each aligned block of 16 rows (0 to 15, 16 to 31, ...) at most 7 rows name the same one
- gate_values: float32 [64, 8], P(('ctx', 'ep')), may hold values from 0.1 to 2.5
- hidden: bfloat16 [4, 32, 7, 1536], P(None, 'ep', None, 'ctx'), may hold values from -0.29882812 to 0.29882812
- w_down: bfloat16 [32, 1536, 3584], P('ep', 'ctx'), may hold values from -0.15625 to 0.15625
Outputs:
- hidden_grad: bfloat16 [4, 32, 7, 1536], P(None, 'ep', None, 'ctx')
- weight_grad: bfloat16 [32, 1536, 3584], P('ep', 'ctx')
- gate_grad: float32 [64, 8], P(('ctx', 'ep'))
The draws below stay inside these ranges and needn't reach their ends.
Inputs may be any that keep to these rules, and one draw needn't show every extreme that they name: `expert_ids`: each token names 8 different experts. In each aligned block of 16 tokens no expert is named by more than 7 tokens.
All inputs are finite; a program needn't handle non-finite values.
Results may differ from the reference program's by a relative error of at most 0.012.
Values may be sent and summed in bfloat16 or wider, within the bound.
No kernel may reach another device: no remote copies, remote signals or barrier semaphores. Data moves between devices by JAX's collectives and lax.ppermute only.
A program may use at most 64 MiB of HBM per device.

```python
import math
import jax
import jax.numpy as jnp
import numpy as np
from jax import lax

D = 3584
F = 1536
TOPK = 8
EXPERTS = 32
CAPACITY = 7
GROUPS = 4
GROUP_TOK = 16
TOKENS = 64


def level_of(stream_key, extent, pieces, low, high):
    factor_of, own = 1.0, jax.random.fold_in(stream_key, 6)
    for axis_at, parts in pieces:
        heights = jnp.exp(jax.random.uniform(jax.random.fold_in(own, axis_at), (parts,), jnp.float32, low / len(pieces), high / len(pieces)))
        factor_of = factor_of * jnp.repeat(heights, extent[axis_at] // parts).reshape([-1 if axis == axis_at else 1 for axis in range(len(extent))])
    return factor_of


def routed_block(key, own, number, rows, amount, top, most, lean):
    order = jax.random.permutation(key, amount)
    heavy_load, common = portions_of(amount, rows * top, most, lean, True), portions_of(amount, rows * top, most, lean, False)
    places = jnp.arange(amount)

    def named(tallies, offset_by):
        used = int((tallies > 0).sum())
        fixed = max(1, used // 4)
        moved = fixed + (places - fixed + offset_by * (used - fixed)) % max(1, amount - fixed)
        return jnp.zeros((amount,), jnp.int32).at[order[jnp.where(places < fixed, places, moved)]].set(jnp.asarray(tallies, jnp.int32))

    tallies = jnp.where(number % 4 == 0, named(heavy_load, number // 4), named(common, number - number // 4 - 1))
    mixed = jax.random.permutation(jax.random.fold_in(own, 3), amount)
    donor, sink = mixed[0:amount // 2 * 2:2], mixed[1:amount // 2 * 2:2]
    room = jnp.minimum(tallies[donor] - 1, most - tallies[sink]) // 2
    room = jnp.where((donor == order[0]) | (sink == order[0]) | (tallies[sink] == 0), 0, jnp.maximum(room, 0))
    moved = jax.random.randint(jax.random.fold_in(own, 4), (amount // 2,), 0, 1 << 20) % (room + 1)
    tallies = tallies.at[donor].add(-moved).at[sink].add(moved)
    labels = jnp.searchsorted(jnp.cumsum(tallies), jnp.arange(rows * top), side="right").astype(jnp.int32)
    table = labels.reshape(top, rows).T
    table = table[jax.random.permutation(jax.random.fold_in(own, 1), rows)]
    offset_by = jax.random.randint(jax.random.fold_in(own, 2), (rows, 1), 0, top)
    return jnp.take_along_axis(table, (jnp.arange(top)[None, :] + offset_by) % top, axis=1)


def portions_of(number_of, total, most, slope, full):
    portions = [(1 << 20) // math.isqrt(standing ** slope) + 1 for standing in range(1, number_of + 1)]
    largest = most if full else min(most, max(-(-total // number_of), total * portions[0] // sum(portions)))
    least = 1 if total - largest >= number_of - 1 else 0
    counts, surplus = [largest] + [least] * (number_of - 1), total - largest - least * (number_of - 1)
    while surplus > 0:
        movable = [i for i in range(1, number_of) if counts[i] < largest] or [i for i in range(1, number_of) if counts[i] < most]
        mass, remaining = sum([portions[i] for i in movable]), surplus
        for i in movable:
            extra = min(most - counts[i], max(1, remaining * portions[i] // mass), surplus)
            counts[i] = counts[i] + extra
            surplus = surplus - extra
    return np.array(counts)


def scatter_about(stream_key, dims, spread, bound, shards=(), kind=jnp.bfloat16):
    values = spread * jax.random.normal(stream_key, dims, jnp.float32)
    if shards:
        values = values * level_of(stream_key, dims, shards, -0.22, 0.18)
    return jnp.clip(values, -bound, bound).astype(kind)


def setup_inputs(seed: int = 0) -> dict:
    splits = jax.random.split(jax.random.key(seed), 6)
    out_grad = scatter_about(splits[0], (TOKENS, D), 1.0, 6.0, ((0, 32),))
    expert_ids_keys = jax.random.split(jax.random.fold_in(splits[1], 1), TOKENS // GROUP_TOK)
    expert_ids_turns = jax.random.permutation(jax.random.fold_in(splits[1], 3), TOKENS // GROUP_TOK)
    expert_ids = jax.vmap(lambda own, number: routed_block(jax.random.fold_in(splits[1], 2), own, number, GROUP_TOK, EXPERTS, TOPK, CAPACITY, 2))(expert_ids_keys, expert_ids_turns).reshape((TOKENS, TOPK))
    gate_values = jnp.clip(jnp.exp(math.log(2.5) - 3.218876 * jax.random.uniform(splits[2], (TOKENS, TOPK), jnp.float32) ** level_of(splits[2], (TOKENS, TOPK), ((0, 32),), -0.2, 0.2)), 0.1, 2.5)
    hidden = scatter_about(splits[3], (GROUPS, EXPERTS, CAPACITY, F), 0.05, 0.29882812, ((1, 8), (3, 4)))
    w_down = scatter_about(splits[4], (EXPERTS, F, D), F ** -0.5, 0.15625, ((0, 8), (1, 4)))
    return {"out_grad": out_grad, "expert_ids": expert_ids, "gate_values": gate_values, "hidden": hidden, "w_down": w_down}


def route_slots(expert_ids):
    group_routes = GROUP_TOK * TOPK
    group_ids = expert_ids.reshape(GROUPS, group_routes)
    onehot = (group_ids[:, :, None] == jnp.arange(EXPERTS, dtype=jnp.int32)[None, None, :]).astype(jnp.int32)
    before = jnp.cumsum(onehot, axis=1) - onehot
    slot_index = jnp.sum(before * onehot, axis=2).astype(jnp.int32)
    return group_ids, slot_index


def reference(out_grad, expert_ids, gate_values, hidden, w_down):
    group_routes = GROUP_TOK * TOPK
    group_ids, slot_index = route_slots(expert_ids)
    place = (group_ids * CAPACITY + slot_index).astype(jnp.int32)
    group_base = (jnp.arange(GROUPS, dtype=jnp.int32) * GROUP_TOK)[:, None]
    token_index = group_base + (jnp.arange(group_routes, dtype=jnp.int32) // TOPK)[None, :]
    group_index = jnp.broadcast_to(jnp.arange(GROUPS, dtype=jnp.int32)[:, None], place.shape)
    slot_token = jnp.zeros((GROUPS, EXPERTS * CAPACITY), jnp.int32).at[group_index, place].set(token_index + 1)
    slot_gate = jnp.zeros((GROUPS, EXPERTS * CAPACITY), jnp.float32).at[group_index, place].set(
        gate_values.reshape(GROUPS, group_routes))
    slot_token = slot_token.reshape(GROUPS, EXPERTS, CAPACITY)
    slot_gate = slot_gate.reshape(GROUPS, EXPERTS, CAPACITY)

    def one_expert(expert):
        token_pick = slot_token[:, expert, :].reshape(-1)
        gate_pick = slot_gate[:, expert, :].reshape(-1)
        live_mask = token_pick > 0
        safe_index = jnp.maximum(token_pick - 1, 0).astype(jnp.int32)
        slot_rows = jnp.where(live_mask[:, None], out_grad[safe_index], jnp.zeros((), out_grad.dtype))
        weight = w_down[expert]
        grad_in = jnp.dot(slot_rows, weight.T, preferred_element_type=jnp.float32)
        saved_hid = hidden[:, expert].reshape(GROUPS * CAPACITY, F)
        hid_grad = (gate_pick[:, None] * grad_in).astype(jnp.bfloat16)
        gate_slot = jnp.sum(saved_hid.astype(jnp.float32) * grad_in, axis=1)
        scaled = (gate_pick[:, None] * slot_rows.astype(jnp.float32)).astype(jnp.bfloat16)
        weight_sum = jnp.dot(saved_hid.T, scaled, preferred_element_type=jnp.float32)
        return hid_grad.reshape(GROUPS, CAPACITY, F), gate_slot.reshape(GROUPS, CAPACITY), weight_sum.astype(jnp.bfloat16)

    hid_all, gate_all, weight_grad = lax.map(one_expert, jnp.arange(EXPERTS, dtype=jnp.int32))
    hidden_grad = jnp.transpose(hid_all, (1, 0, 2, 3))
    gate_table = jnp.transpose(gate_all, (1, 0, 2)).reshape(GROUPS, EXPERTS * CAPACITY)
    gate_grad = jnp.take_along_axis(gate_table, place, axis=1).reshape(TOKENS, TOPK)
    return hidden_grad, weight_grad, gate_grad
```

```python
import jax
import jax.numpy as jnp
from jax import lax
from jax.experimental import pallas as pl
from jax.experimental.pallas import tpu as pltpu
from jax.sharding import PartitionSpec as P

LANES = 128
DIRECT_MAX = 8


def gather_tokens(packed):
    ctx_count = lax.axis_size("ctx")
    if ctx_count <= DIRECT_MAX:
        blocks = [packed] + [
            lax.ppermute(packed, "ctx", [(i, (i + step) % ctx_count) for i in range(ctx_count)])
            for step in range(1, ctx_count)
        ]
        stacked = jnp.stack(blocks)
        block_group = (lax.axis_index("ctx") - jnp.arange(ctx_count)) % ctx_count
    else:
        stacked = lax.all_gather(packed, "ctx", axis=0)
        block_group = jnp.arange(ctx_count)
    return lax.all_gather(stacked, "ep", axis=0), block_group.astype(jnp.int32)


def expert_kernel(model_width):
    def body(rows_ref, key_ref, gate_ref, hidden_ref, w_ref, hid_grad_ref, gate_piece_ref, w_grad_ref):
        slots = hidden_ref.shape[1]
        key = key_ref[0]
        place = lax.broadcasted_iota(jnp.int32, (slots, key.shape[1]), 0)
        pick = place == key
        slot_gate = jnp.sum(jnp.where(pick, gate_ref[0], 0.0), axis=1, keepdims=True)
        rows = jnp.dot(
            pick.astype(jnp.float32).astype(jnp.bfloat16),
            rows_ref[:, :model_width],
            preferred_element_type=jnp.float32,
        )
        rows_bf = rows.astype(jnp.bfloat16)
        hidden = hidden_ref[0]
        grad_in = lax.dot_general(
            rows_bf, w_ref[0], (((1,), (1,)), ((), ())), preferred_element_type=jnp.float32
        )
        hid_grad_ref[0] = (slot_gate * grad_in).astype(jnp.bfloat16)
        slot_term = jnp.sum(hidden.astype(jnp.float32) * grad_in, axis=1, keepdims=True)
        gate_piece_ref[0] = jnp.sum(jnp.where(pick, slot_term, 0.0), axis=0, keepdims=True)
        scaled = (slot_gate * rows).astype(jnp.bfloat16)
        w_grad_ref[0] = lax.dot_general(
            hidden, scaled, (((0,), (0,)), ((), ())), preferred_element_type=jnp.float32
        ).astype(jnp.bfloat16)

    return body


def per_device(out_grad, expert_ids, gate_values, hidden, w_down):
    tok_dev, top_count = expert_ids.shape
    groups, exp_dev, capacity, width_part = hidden.shape
    model_width = out_grad.shape[1]
    ep_count, ctx_count = lax.axis_size("ep"), lax.axis_size("ctx")
    ep_rank = lax.axis_index("ep")
    tokens = ep_count * ctx_count * tok_dev
    slots = groups * capacity
    assert exp_dev * ep_count <= 256 and 3 * top_count <= LANES

    gate_hi = gate_values.astype(jnp.bfloat16)
    gate_lo = (gate_values - gate_hi.astype(jnp.float32)).astype(jnp.bfloat16)
    packed = jnp.concatenate(
        [
            out_grad,
            expert_ids.astype(jnp.bfloat16),
            gate_hi,
            gate_lo,
            jnp.zeros((tok_dev, LANES - 3 * top_count), jnp.bfloat16),
        ],
        axis=1,
    )
    gathered, block_group = gather_tokens(packed)
    rows = gathered.reshape(tokens, model_width + LANES)
    extra = gathered[..., model_width:].astype(jnp.float32)
    ids = extra[..., :top_count].astype(jnp.int32)
    gates = extra[..., top_count : 2 * top_count] + extra[..., 2 * top_count : 3 * top_count]

    own_experts = ep_rank * exp_dev + jnp.arange(exp_dev, dtype=jnp.int32)
    named = ids[None] == own_experts[:, None, None, None, None]
    hit = jnp.any(named, axis=4)
    token_gate = jnp.sum(jnp.where(named, gates[None], 0.0), axis=4)
    order = jnp.arange(ep_count * tok_dev, dtype=jnp.int32)
    earlier = (order[:, None] < order[None, :]).reshape(ep_count, tok_dev, ep_count, tok_dev)
    slot = jnp.sum(
        jnp.where(
            hit[:, :, :, :, None, None] & earlier[None, :, None, :, :, :], 1, 0
        ).astype(jnp.int32),
        axis=(1, 3),
    )
    slot = jnp.transpose(slot, (0, 2, 1, 3))
    key = jnp.where(hit, block_group[None, None, :, None] * capacity + slot, -1)

    hidden_e = jnp.transpose(hidden, (1, 0, 2, 3)).reshape(exp_dev, slots, width_part)
    per_expert = lambda *shape: pl.BlockSpec((1,) + shape, lambda e: (e, 0, 0))
    hid_grad, gate_piece, w_grad = pl.pallas_call(
        expert_kernel(model_width),
        grid=(exp_dev,),
        in_specs=[
            pl.BlockSpec(memory_space=pltpu.VMEM),
            per_expert(1, tokens),
            per_expert(1, tokens),
            per_expert(slots, width_part),
            per_expert(width_part, model_width),
        ],
        out_specs=[
            per_expert(slots, width_part),
            per_expert(1, tokens),
            per_expert(width_part, model_width),
        ],
        out_shape=[
            jax.ShapeDtypeStruct((exp_dev, slots, width_part), jnp.bfloat16),
            jax.ShapeDtypeStruct((exp_dev, 1, tokens), jnp.float32),
            jax.ShapeDtypeStruct((exp_dev, width_part, model_width), jnp.bfloat16),
        ],
        compiler_params=pltpu.CompilerParams(vmem_limit_bytes=56 * 1024 * 1024),
    )(
        rows,
        key.reshape(exp_dev, 1, tokens),
        token_gate.reshape(exp_dev, 1, tokens),
        hidden_e,
        w_down,
    )
    hidden_grad = jnp.transpose(
        hid_grad.reshape(exp_dev, groups, capacity, width_part), (1, 0, 2, 3)
    )

    piece = gate_piece.reshape(exp_dev, ep_count, ctx_count, tok_dev)
    at_group = block_group[None, :] == jnp.arange(ctx_count, dtype=jnp.int32)[:, None]
    sends = jnp.sum(
        jnp.where(at_group[:, :, None, None, None], jnp.transpose(piece, (2, 1, 3, 0))[None], 0.0),
        axis=1,
    )
    sends = sends.reshape(ctx_count * ep_count, tok_dev * exp_dev)
    parts = lax.all_to_all(sends, ("ctx", "ep"), 0, 0, tiled=True)
    table = jnp.sum(parts.reshape(ctx_count, ep_count, tok_dev, exp_dev), axis=0)
    table = jnp.transpose(table, (1, 0, 2)).reshape(tok_dev, 1, ep_count * exp_dev)
    all_experts = jnp.arange(ep_count * exp_dev, dtype=jnp.int32)
    lookup = expert_ids[:, :, None] == all_experts[None, None, :]
    gate_grad = jnp.sum(jnp.where(lookup, table, 0.0), axis=2)
    return (hidden_grad, w_grad, gate_grad)


def solution(mesh):
    placed = (
        P(("ctx", "ep"), None),
        P(("ctx", "ep"), None),
        P(("ctx", "ep"), None),
        P(None, "ep", None, "ctx"),
        P("ep", "ctx", None),
    )
    return jax.shard_map(
        per_device,
        mesh=mesh,
        in_specs=placed,
        out_specs=(P(None, "ep", None, "ctx"), P("ep", "ctx", None), P(("ctx", "ep"), None)),
        check_vma=False,
    )
```

```python
import jax
import jax.numpy as jnp
from jax import lax
from jax.experimental import pallas as pl
from jax.experimental.pallas import tpu as pltpu
from jax.sharding import PartitionSpec as P

LANES = 128
DIRECT_MAX = 8


def gather_tokens(packed):
    ctx_count = lax.axis_size("ctx")
    if ctx_count <= DIRECT_MAX:
        blocks = [packed] + [
            lax.ppermute(packed, "ctx", [(i, (i + step) % ctx_count) for i in range(ctx_count)])
            for step in range(1, ctx_count)
        ]
        stacked = jnp.stack(blocks)
        block_group = (lax.axis_index("ctx") - jnp.arange(ctx_count)) % ctx_count
    else:
        stacked = lax.all_gather(packed, "ctx", axis=0)
        block_group = jnp.arange(ctx_count)
    return lax.all_gather(stacked, "ep", axis=0), block_group.astype(jnp.int32)


def pack_kernel(grad_ref, ids_ref, gate_ref, packed_ref):
    tok_dev, model_width = grad_ref.shape
    gate = gate_ref[...]
    gate_hi = gate.astype(jnp.bfloat16).astype(jnp.float32)
    gate_lo = gate - gate_hi
    parts = [ids_ref[...].astype(jnp.float32), gate_hi, gate_lo]
    spare = LANES - sum(part.shape[1] for part in parts)
    parts.append(jnp.zeros((tok_dev, spare), jnp.float32))
    packed_ref[:, :model_width] = grad_ref[...]
    packed_ref[:, model_width:] = jnp.concatenate(parts, axis=1).astype(jnp.bfloat16)


def grad_in_kernel(sizes):
    model_width, top_count, capacity, ctx_count, ep_count, tok_dev, rotated = sizes

    def body(
        place_ref, rows_ref, hidden_ref, w_hbm, hid_grad_ref, sends_ref, scaled_ref, w_ref, arrived
    ):
        tokens = rows_ref.shape[0]
        exp_dev, slots, _ = hidden_ref.shape
        slot_lanes = -(-slots // LANES) * LANES
        first_expert = place_ref[0]
        fetches = [
            pltpu.make_async_copy(w_hbm.at[e], w_ref.at[e], arrived.at[e]) for e in range(exp_dev)
        ]
        for fetch in fetches:
            fetch.start()
        extra = rows_ref[:, model_width:].astype(jnp.float32)
        lane = lax.broadcasted_iota(jnp.int32, extra.shape, 1)

        def block_and_order(index):
            pair = index // tok_dev
            lap = pair // ctx_count
            return pair - lap * ctx_count, lap * tok_dev + (index - pair * tok_dev)

        late = block_and_order(lax.broadcasted_iota(jnp.int32, (tokens, tokens), 0))
        soon = block_and_order(lax.broadcasted_iota(jnp.int32, (tokens, tokens), 1))
        earlier = jnp.where((late[0] == soon[0]) & (soon[1] < late[1]), 1.0, 0.0)
        block = block_and_order(lax.broadcasted_iota(jnp.int32, (tokens, 1), 0))[0]
        group = block
        if rotated:
            group = place_ref[1] - block
            group = jnp.where(group < 0, group + ctx_count, group)
        hits, gates = [], []
        all_hits = jnp.zeros(extra.shape, jnp.float32)
        for e in range(exp_dev):
            expert = (first_expert + e).astype(jnp.float32)
            named = jnp.where((extra == expert) & (lane < top_count), 1.0, 0.0)
            at_gates = pltpu.roll(named, top_count, 1) + pltpu.roll(named, 2 * top_count, 1)
            hits.append(jnp.sum(named, axis=1, keepdims=True))
            gates.append(jnp.sum(at_gates * extra, axis=1, keepdims=True))
            all_hits = jnp.where(lane == e, hits[e], all_hits)
        counts = jnp.dot(
            earlier.astype(jnp.bfloat16),
            all_hits.astype(jnp.bfloat16),
            preferred_element_type=jnp.float32,
        )
        slot_lane = lax.broadcasted_iota(jnp.int32, (tokens, slot_lanes), 1)
        row = lax.broadcasted_iota(jnp.int32, (slots, 1), 0)
        row_group = row // capacity
        row_slot = row - row_group * capacity
        send_lane = lax.broadcasted_iota(jnp.int32, (slots, sends_ref.shape[1]), 1)
        placed = jnp.zeros((slots, sends_ref.shape[1]), jnp.float32)
        for e in range(exp_dev):
            key = group * capacity + counts[:, e : e + 1].astype(jnp.int32)
            key = jnp.where(hits[e] > 0.0, key, -1)
            pick_t = jnp.where(key == slot_lane, 1.0, 0.0)
            pick = pick_t.T[:slots]
            slot_gate = jnp.sum((pick_t * gates[e]).T, axis=1, keepdims=True)[:slots]
            rows = jnp.dot(
                pick.astype(jnp.bfloat16),
                rows_ref[:, :model_width],
                preferred_element_type=jnp.float32,
            )
            scaled_ref[e] = (slot_gate * rows).astype(jnp.bfloat16)
            fetches[e].wait()
            grad_in = lax.dot_general(
                rows.astype(jnp.bfloat16),
                w_ref[e],
                (((1,), (1,)), ((), ())),
                preferred_element_type=jnp.float32,
            )
            hid_grad_ref[e] = (slot_gate * grad_in).astype(jnp.bfloat16)
            term = jnp.sum(hidden_ref[e].astype(jnp.float32) * grad_in, axis=1, keepdims=True)
            placed = placed + jnp.where(send_lane == row_slot + e * capacity, term, 0.0)
        for n in range(ctx_count):
            line = jnp.sum(jnp.where(row_group == n, placed, 0.0), axis=0, keepdims=True)
            sends_ref[n * ep_count : (n + 1) * ep_count] = jnp.broadcast_to(
                line, (ep_count, sends_ref.shape[1])
            )

    return body


def outer_kernel(hidden_ref, scaled_ref, w_grad_ref):
    w_grad_ref[0] = lax.dot_general(
        hidden_ref[0], scaled_ref[0], (((0,), (0,)), ((), ())), preferred_element_type=jnp.float32
    ).astype(jnp.bfloat16)


def per_device(out_grad, expert_ids, gate_values, hidden, w_down):
    tok_dev, top_count = expert_ids.shape
    groups, exp_dev, capacity, width_part = hidden.shape
    model_width = out_grad.shape[1]
    ep_count, ctx_count = lax.axis_size("ep"), lax.axis_size("ctx")
    ep_rank, ctx_rank = lax.axis_index("ep"), lax.axis_index("ctx")
    tokens = ep_count * ctx_count * tok_dev
    slots = groups * capacity
    send_width = -(-exp_dev * capacity // LANES) * LANES
    assert exp_dev * ep_count <= 256 and 3 * top_count <= LANES and groups == ctx_count
    vmem = pl.BlockSpec(memory_space=pltpu.VMEM)
    held = 2 * (tokens + exp_dev * slots) * (model_width + LANES)
    limit = pltpu.CompilerParams(vmem_limit_bytes=min(56 << 20, (16 << 20) + 2 * w_down.size + 3 * held))

    packed = pl.pallas_call(
        pack_kernel,
        in_specs=[vmem, vmem, vmem],
        out_specs=vmem,
        out_shape=jax.ShapeDtypeStruct((tok_dev, model_width + LANES), jnp.bfloat16),
    )(out_grad, expert_ids, gate_values)
    gathered, block_group = gather_tokens(packed)
    rows = gathered.reshape(tokens, model_width + LANES)
    rotated = ctx_count <= DIRECT_MAX
    hidden_e = jnp.transpose(hidden, (1, 0, 2, 3)).reshape(exp_dev, slots, width_part)
    sizes = (model_width, top_count, capacity, ctx_count, ep_count, tok_dev, rotated)
    place = jnp.stack([ep_rank * exp_dev, ctx_rank]).astype(jnp.int32)
    flops = 2 * exp_dev * slots * width_part * model_width
    hid_grad, sends, scaled = pl.pallas_call(
        grad_in_kernel(sizes),
        in_specs=[pl.BlockSpec(memory_space=pltpu.SMEM), vmem, vmem, pl.BlockSpec(memory_space=pl.ANY)],
        out_specs=[vmem, vmem, vmem],
        out_shape=[
            jax.ShapeDtypeStruct((exp_dev, slots, width_part), jnp.bfloat16),
            jax.ShapeDtypeStruct((ctx_count * ep_count, send_width), jnp.float32),
            jax.ShapeDtypeStruct((exp_dev, slots, model_width), jnp.bfloat16),
        ],
        scratch_shapes=[
            pltpu.VMEM(w_down.shape, w_down.dtype),
            pltpu.SemaphoreType.DMA((exp_dev,)),
        ],
        compiler_params=limit,
        cost_estimate=pl.CostEstimate(flops=20 * flops, bytes_accessed=0, transcendentals=0),
    )(place, rows, hidden_e, w_down)

    parts = lax.all_to_all(sends, ("ctx", "ep"), 0, 0, tiled=True)
    per_expert = lambda *shape: pl.BlockSpec((1,) + shape, lambda e: (e, 0, 0))
    w_grad = pl.pallas_call(
        outer_kernel,
        grid=(exp_dev,),
        in_specs=[per_expert(slots, width_part), per_expert(slots, model_width)],
        out_specs=per_expert(width_part, model_width),
        out_shape=jax.ShapeDtypeStruct((exp_dev, width_part, model_width), jnp.bfloat16),
        compiler_params=limit,
        cost_estimate=pl.CostEstimate(
            flops=20 * flops, bytes_accessed=w_down.size * 2, transcendentals=0
        ),
    )(hidden_e, scaled)
    hidden_grad = jnp.transpose(
        hid_grad.reshape(exp_dev, groups, capacity, width_part), (1, 0, 2, 3)
    )

    own_at = 0 if rotated else ctx_rank
    own_block = lax.dynamic_index_in_dim(gathered, own_at, 1, False)
    group_ids = own_block[:, :, model_width : model_width + top_count].astype(jnp.int32)
    order = jnp.arange(ep_count * tok_dev, dtype=jnp.int32).reshape(ep_count, tok_dev)
    own_order = ep_rank * tok_dev + jnp.arange(tok_dev, dtype=jnp.int32)
    before = order[None] < own_order[:, None, None]
    same = group_ids[None, None] == expert_ids[:, :, None, None, None]
    own_slot = jnp.sum((same & before[:, None, :, :, None]).astype(jnp.int32), axis=(2, 3, 4))
    home = expert_ids // exp_dev
    at_lane = (expert_ids - home * exp_dev) * capacity + own_slot
    found = (home[:, :, None, None] == jnp.arange(ep_count, dtype=jnp.int32)[:, None]) & (
        at_lane[:, :, None, None] == jnp.arange(send_width, dtype=jnp.int32)[None, :]
    )
    table = jnp.sum(parts.reshape(ctx_count, ep_count, send_width), axis=0)
    gate_grad = jnp.sum(jnp.where(found, table[None, None], 0.0), axis=(2, 3))
    return (hidden_grad, w_grad, gate_grad)


def solution(mesh):
    placed = (
        P(("ctx", "ep"), None),
        P(("ctx", "ep"), None),
        P(("ctx", "ep"), None),
        P(None, "ep", None, "ctx"),
        P("ep", "ctx", None),
    )
    return jax.shard_map(
        per_device,
        mesh=mesh,
        in_specs=placed,
        out_specs=(P(None, "ep", None, "ctx"), P("ep", "ctx", None), P(("ctx", "ep"), None)),
        check_vma=False,
    )
```
